32 devices in a mesh: gx: 8 (over z, x), col: 4 (over y, core).
Axes of the slice: x: 2, y: 2, z: 4, core: 2. Of those that a mesh axis runs over, the one named last changes fastest.
Arguments:
- grid_field: bfloat16 [64, 32, 256, 128], P('col', 'gx'), may hold values from -6 to 6
- tucker_core: float32 [2, 32, 32, 8, 8, 4], P(None, 'col'), may hold values from -0.5 to 0.5
- in_factor: float32 [64, 32], P('col'), may hold values from -0.75 to 0.75
- out_factor: float32 [64, 32], P('col'), may hold values from -1 to 1
- x_factor: float32 [32, 8], replicated, may hold values from -4 to 4
- y_factor: float32 [32, 8], replicated, may hold values from -4 to 4
- z_factor: float32 [16, 4], replicated, may hold values from -4 to 4
- kx_reach: int32 [32, 16], replicated, may hold values from 1 to 17
Outputs:
- spectral_out: bfloat16 [64, 32, 256, 128], P('col', 'gx')
The draws below stay inside these ranges and needn't reach their ends.
All inputs are finite; a program needn't handle non-finite values.
Results may differ from the reference program's by a relative error of at most 0.001.
Values sent between devices are 32-bit elements; how exact they have to be, the bound alone decides.
A program may use at most 64 MiB of HBM per device.

```python
import jax
import jax.numpy as jnp
from jax import lax

C = 64
R_IN = 32
R_OUT = 32
RX = 8
RY = 8
RZ = 4
KX = 32
KY = 32
KZ = 16
NY = 256
NZ = 128
NX = 32


def set_ends(result, key, low, top_value):
    dims = result.shape
    spot = [jax.random.randint(jax.random.fold_in(key, axis), (), 0, dims[axis]) for axis in range(len(dims))]
    result = result.at[tuple(spot)].set(low)
    longest = dims.index(max(dims))
    spot[longest] = (spot[longest] + 1) % dims[longest]
    return result.at[tuple(spot)].set(top_value)


def steps_of(key, shape, split, low, top_value):
    loudness, own = 1.0, jax.random.fold_in(key, 6)
    for axis_at, shards_of in split:
        steps = jnp.exp(jax.random.uniform(jax.random.fold_in(own, axis_at), (shards_of,), jnp.float32, low / len(split), top_value / len(split)))
        loudness = loudness * jnp.repeat(steps, shape[axis_at] // shards_of).reshape([-1 if axis == axis_at else 1 for axis in range(len(shape))])
    return loudness


def noise(own_key, extent, scale, reach, pieces=(), kind=jnp.bfloat16):
    values = jax.random.normal(own_key, extent, jnp.float32) * scale
    if len(pieces) > 0:
        values = steps_of(own_key, extent, pieces, -0.22, 0.18) * values
    return jnp.clip(values, min=-reach, max=reach).astype(kind)


def setup_inputs(seed: int = 0) -> dict:
    streams_of = jax.random.split(jax.random.key(seed), 9)
    grid_field = noise(streams_of[0], (C, NX, NY, NZ), 1.0, 6.0, ((0, 4), (1, 8)))
    tucker_core = noise(streams_of[1], (2, R_IN, R_OUT, RX, RY, RZ), (max(1, KX * KY * KZ * R_IN * RX * RY * RZ // (NX * NY * NZ))) ** -0.5, 0.5, ((1, 4),), jnp.float32)
    in_factor = noise(streams_of[2], (C, R_IN), C ** -0.5, 0.75, ((0, 4),), jnp.float32)
    out_factor = noise(streams_of[3], (C, R_OUT), R_OUT ** -0.5, 1.0, ((0, 4),), jnp.float32)
    x_factor = noise(streams_of[4], (KX, RX), 1.0, 4.0, (), jnp.float32)
    y_factor = noise(streams_of[5], (KY, RY), 1.0, 4.0, (), jnp.float32)
    z_factor = noise(streams_of[6], (KZ, RZ), 1.0, 4.0, (), jnp.float32)
    kx_reach = set_ends(jax.random.randint(streams_of[7], (KY, KZ), 1, KX // 2 + 2), jax.random.fold_in(streams_of[7], 1), 1, (KX // 2 + 2) - 1).astype(jnp.int32)
    return {"grid_field": grid_field, "tucker_core": tucker_core, "in_factor": in_factor, "out_factor": out_factor, "x_factor": x_factor, "y_factor": y_factor, "z_factor": z_factor, "kx_reach": kx_reach}


def slot_freq(slot_count):
    slot_index = jnp.arange(slot_count, dtype=jnp.int32)
    return jnp.where(slot_index < slot_count // 2, slot_index, slot_index - slot_count)


def forward_one(channel):
    values = channel.astype(jnp.float32)
    spectrum = jnp.fft.rfft(values, axis=2, norm="ortho")[:, :, :KZ]
    spectrum = jnp.fft.fft(spectrum, axis=1, norm="ortho")
    spectrum = jnp.concatenate([spectrum[:, :KY // 2], spectrum[:, NY - KY // 2:]], axis=1)
    spectrum = jnp.fft.fft(spectrum, axis=0, norm="ortho")
    spectrum = jnp.concatenate([spectrum[:KX // 2], spectrum[NX - KX // 2:]], axis=0)
    return jnp.real(spectrum), jnp.imag(spectrum)


def inverse_one(pair_parts):
    real_part, imag_part = pair_parts
    values = real_part + 1j * imag_part
    zero_fill = jnp.zeros((NX - KX, KY, KZ), values.dtype)
    values = jnp.concatenate([values[:KX // 2], zero_fill, values[KX // 2:]], axis=0)
    values = jnp.fft.ifft(values, axis=0, norm="ortho")
    zero_fill = jnp.zeros((NX, NY - KY, KZ), values.dtype)
    values = jnp.concatenate([values[:, :KY // 2], zero_fill, values[:, KY // 2:]], axis=1)
    values = jnp.fft.ifft(values, axis=1, norm="ortho")
    zero_fill = jnp.zeros((NX, NY, NZ // 2 + 1 - KZ), values.dtype)
    values = jnp.concatenate([values, zero_fill], axis=2)
    return jnp.fft.irfft(values, n=NZ, axis=2, norm="ortho").astype(jnp.bfloat16)


def reference(grid_field, tucker_core, in_factor, out_factor, x_factor, y_factor, z_factor, kx_reach):
    highest = lax.Precision.HIGHEST
    real_spec, imag_spec = lax.map(forward_one, grid_field)
    kept_mask = (jnp.abs(slot_freq(KX))[:, None, None] < kx_reach[None, :, :]).astype(jnp.float32)
    rank_re = jnp.einsum('cr,cijl->rijl', in_factor, real_spec, precision=highest) * kept_mask
    rank_im = jnp.einsum('cr,cijl->rijl', in_factor, imag_spec, precision=highest) * kept_mask

    def per_row(row_items):
        row_re, row_im, y_row = row_items
        partial_value = jnp.einsum('prsabe,b->prsae', tucker_core, y_row, precision=highest)
        kernel = jnp.einsum('prsae,ia,le->prsil', partial_value, x_factor, z_factor, precision=highest)
        mixed_re = (jnp.einsum('rsil,ril->sil', kernel[0], row_re, precision=highest)
                    - jnp.einsum('rsil,ril->sil', kernel[1], row_im, precision=highest))
        mixed_im = (jnp.einsum('rsil,ril->sil', kernel[0], row_im, precision=highest)
                    + jnp.einsum('rsil,ril->sil', kernel[1], row_re, precision=highest))
        out_re = jnp.einsum('os,sil->oil', out_factor, mixed_re, precision=highest)
        out_im = jnp.einsum('os,sil->oil', out_factor, mixed_im, precision=highest)
        return out_re, out_im

    out_re, out_im = lax.map(per_row, (jnp.moveaxis(rank_re, 2, 0), jnp.moveaxis(rank_im, 2, 0), y_factor))
    out_re = jnp.transpose(out_re, (1, 2, 0, 3))
    out_im = jnp.transpose(out_im, (1, 2, 0, 3))
    return lax.map(inverse_one, (out_re, out_im))
```

```python
import functools
import math

import jax
import jax.numpy as jnp
import numpy as np
from jax import lax
from jax.experimental import pallas as pl
from jax.experimental.pallas import tpu as pltpu
from jax.sharding import PartitionSpec as P

MESH = pl.DeviceIdType.MESH
VMEM = pl.BlockSpec(memory_space=pltpu.VMEM)
F32 = jnp.float32
BF16 = jnp.bfloat16


def slot_freq(slot_count):
    slot_index = jnp.arange(slot_count, dtype=jnp.int32)
    return jnp.where(slot_index < slot_count // 2, slot_index, slot_index - slot_count)


def phase_table(positions, extent, slot_count, direction):
    phase_steps = positions[:, None] * slot_freq(slot_count)[None, :] % extent
    radians = 2.0 * math.pi / extent * phase_steps.astype(jnp.float32)
    norm_scale = 1.0 / math.sqrt(extent)
    cosine = jnp.cos(radians) * norm_scale
    sine_part = direction * jnp.sin(radians) * norm_scale
    return jnp.stack([jnp.stack([cosine, -sine_part], 1), jnp.stack([sine_part, cosine], 1)], 1)


def z_tables(grid_z, modes_z):
    z_index = jnp.arange(grid_z, dtype=jnp.int32)
    kz_index = jnp.arange(modes_z, dtype=jnp.int32)
    phase_steps = z_index[:, None] * kz_index[None, :] % grid_z
    radians = 2.0 * math.pi / grid_z * phase_steps.astype(jnp.float32)
    norm_scale = 1.0 / math.sqrt(grid_z)
    cosine = jnp.cos(radians) * norm_scale
    sine_part = jnp.sin(radians) * norm_scale
    forward = jnp.stack([cosine, -sine_part], 1)
    weight = jnp.where(kz_index == 0, 1.0, 2.0).astype(jnp.float32)
    backward = jnp.stack([(cosine * weight[None, :]).T, -(sine_part * weight[None, :]).T], 0)
    return (forward, backward)


def plain_device(
    grid_field, tucker_core, in_factor, out_factor, x_factor, y_factor, z_factor, kx_reach
):
    highest = lax.Precision.HIGHEST
    channels, planes, grid_y, grid_z = grid_field.shape
    modes_x = x_factor.shape[0]
    modes_y = y_factor.shape[0]
    modes_z = z_factor.shape[0]
    width_gx = lax.axis_size("gx")
    grid_x = planes * width_gx
    columns = modes_y * modes_z
    col_dev = columns // width_gx
    slab_index = lax.axis_index("gx")
    z_forward, z_backward = z_tables(grid_z, modes_z)
    y_forward = phase_table(jnp.arange(grid_y, dtype=jnp.int32), grid_y, modes_y, 1.0)
    x_forward = phase_table(jnp.arange(grid_x, dtype=jnp.int32), grid_x, modes_x, 1.0)
    values = grid_field.astype(jnp.float32)
    z_spectrum = jnp.einsum("cxyz,zpl->cxply", values, z_forward, precision=highest)
    y_spectrum = jnp.einsum("cxply,ypqj->qcxjl", z_spectrum, y_forward, precision=highest)
    y_spectrum = y_spectrum.reshape(2, channels, planes, columns)
    first_col = slab_index * col_dev
    reach_dev = lax.dynamic_slice_in_dim(kx_reach.reshape(-1), first_col, col_dev)
    kept_mask = (jnp.abs(slot_freq(modes_x))[:, None] < reach_dev[None, :]).astype(jnp.float32)
    arrived = lax.all_to_all(y_spectrum, "gx", split_axis=3, concat_axis=2, tiled=True)
    spectrum = jnp.einsum("pcxm,xpqk->qckm", arrived, x_forward, precision=highest)
    partial_value = jnp.einsum("qckm,cr->qrkm", spectrum, in_factor, precision=highest)
    amplitude = lax.psum_scatter(partial_value, "col", scatter_dimension=1, tiled=True)
    amplitude = amplitude * kept_mask[None, None]
    column = first_col + jnp.arange(col_dev, dtype=jnp.int32)
    pick_y = (column[:, None] // modes_z == jnp.arange(modes_y, dtype=jnp.int32)[None, :]).astype(
        jnp.float32
    )
    pick_z = (column[:, None] % modes_z == jnp.arange(modes_z, dtype=jnp.int32)[None, :]).astype(
        jnp.float32
    )
    y_rows = jnp.dot(pick_y, y_factor, precision=highest)
    z_rows = jnp.dot(pick_z, z_factor, precision=highest)
    core_cols = jnp.einsum("prsabe,mb,me->prsam", tucker_core, y_rows, z_rows, precision=highest)
    kernel = jnp.einsum("prsam,ka->prskm", core_cols, x_factor, precision=highest)
    mixed_re = jnp.einsum("rskm,rkm->skm", kernel[0], amplitude[0], precision=highest) - jnp.einsum(
        "rskm,rkm->skm", kernel[1], amplitude[1], precision=highest
    )
    mixed_im = jnp.einsum("rskm,rkm->skm", kernel[0], amplitude[1], precision=highest) + jnp.einsum(
        "rskm,rkm->skm", kernel[1], amplitude[0], precision=highest
    )
    mixed_sum = lax.psum(jnp.stack([mixed_re, mixed_im]), "col")
    out_spec = jnp.einsum("os,qskm->qokm", out_factor, mixed_sum, precision=highest)
    x_backward = phase_table(jnp.arange(grid_x, dtype=jnp.int32), grid_x, modes_x, -1.0)
    x_values = jnp.einsum("pckm,xpqk->qcxm", out_spec, x_backward, precision=highest)
    returned = lax.all_to_all(x_values, "gx", split_axis=2, concat_axis=3, tiled=True)
    returned = returned.reshape(2, channels, planes, modes_y, modes_z)
    y_backward = phase_table(jnp.arange(grid_y, dtype=jnp.int32), grid_y, modes_y, -1.0)
    y_values = jnp.einsum("pcxjl,ypqj->cxqly", returned, y_backward, precision=highest)
    result = jnp.einsum("cxqly,qlz->cxyz", y_values, z_backward, precision=highest)
    return result.astype(jnp.bfloat16)


def split_np(table):
    high = table.astype(np.float32).astype(BF16)
    low = (table - high.astype(np.float64)).astype(np.float32).astype(BF16)
    return high, low


def split(values):
    high = values.astype(BF16)
    return high, (values - high.astype(F32)).astype(BF16)


def freqs(slots):
    index = np.arange(slots)
    return np.where(index < slots // 2, index, index - slots)


def waves(extent, frequencies):
    steps = np.arange(extent)[:, None] * frequencies[None, :] % extent
    angle = 2.0 * np.pi / extent * steps
    return np.cos(angle) / math.sqrt(extent), np.sin(angle) / math.sqrt(extent)


def dot(a, b):
    return jnp.dot(a, b, preferred_element_type=F32)


def forward_tables(grid_y, grid_z, modes_y, modes_z, planes):
    cos_y, sin_y = waves(grid_y, freqs(modes_y))
    high, low = split_np(np.concatenate([cos_y.T, -sin_y.T], 0))
    y_table = np.concatenate([high, low], 0)
    cos_z, sin_z = waves(grid_z, np.arange(modes_z))
    table = np.zeros((planes, 2, grid_z, modes_z, planes, 2))
    for plane in range(planes):
        table[plane, 0, :, :, plane, 0] = cos_z
        table[plane, 0, :, :, plane, 1] = -sin_z
        table[plane, 1, :, :, plane, 0] = sin_z
        table[plane, 1, :, :, plane, 1] = cos_z
    high, low = split_np(table.reshape(planes * 2 * grid_z, -1))
    return y_table, np.concatenate([high, low], 1)


def inverse_tables(grid_y, grid_z, modes_y, modes_z, planes):
    cos_y, sin_y = waves(grid_y, freqs(modes_y))
    high, low = split_np(np.concatenate([cos_y, -sin_y], 1))
    y_table = np.concatenate([high, high, low], 1)
    cos_z, sin_z = waves(grid_z, np.arange(modes_z))
    weight = np.where(np.arange(modes_z) == 0, 1.0, 2.0)
    cos_z, sin_z = (cos_z * weight).T, (sin_z * weight).T
    table = np.zeros((modes_z, planes, 2, planes, 2, grid_z))
    for plane in range(planes):
        table[:, plane, 0, plane, 0, :] = cos_z
        table[:, plane, 1, plane, 0, :] = -sin_z
        table[:, plane, 0, plane, 1, :] = sin_z
        table[:, plane, 1, plane, 1, :] = cos_z
    high, low = split_np(table.reshape(modes_z * planes * 2, -1))
    return y_table, high, low


def x_tables(grid_x, modes_x):
    cos_x, sin_x = waves(grid_x, freqs(modes_x))
    real = np.stack([cos_x.T, sin_x.T], 2).reshape(modes_x, -1)
    imag = np.stack([-sin_x.T, cos_x.T], 2).reshape(modes_x, -1)
    high, low = split_np(np.concatenate([real, imag, -imag, real], 0))
    forward = np.concatenate([high, high, low], 1)
    real = np.concatenate([cos_x, -sin_x], 1)
    imag = np.concatenate([sin_x, cos_x], 1)
    high, low = split_np(np.stack([real, imag], 1).reshape(grid_x * 2, -1))
    backward = np.concatenate([high, high, low], 1)
    return forward, backward


def forward_kernel(field_ref, y_ref, z_ref, out_ref, high_ref, low_ref):
    channel = pl.program_id(0)
    channels = pl.num_programs(0)
    planes, modes_y = field_ref.shape[1], out_ref.shape[0]
    half = 2 * modes_y
    parts = []
    for plane in range(planes):
        both = dot(y_ref[...], field_ref[0, plane])
        y_values = both[:half] + both[half:]
        parts += [y_values[:modes_y], y_values[modes_y:]]
    high, low = split(jnp.concatenate(parts, 1))
    rows = pl.ds(pl.multiple_of(channel * modes_y, modes_y), modes_y)
    high_ref[rows] = high
    low_ref[rows] = low

    @pl.when(channel == channels - 1)
    def _():
        lanes = out_ref.shape[2]
        both = dot(high_ref[...], z_ref[...])
        result = both[:, :lanes] + both[:, lanes:] + dot(low_ref[...], z_ref[:, :lanes])
        out_ref[...] = jnp.swapaxes(result.reshape(-1, modes_y, lanes), 0, 1)


def forward(grid_field, modes_y, modes_z):
    channels, planes, grid_y, grid_z = grid_field.shape
    y_table, z_table = forward_tables(grid_y, grid_z, modes_y, modes_z, planes)
    lanes = planes * 2 * modes_z
    wide = planes * 2 * grid_z
    return pl.pallas_call(
        forward_kernel,
        grid=(channels,),
        in_specs=[
            pl.BlockSpec((1, planes, grid_y, grid_z), lambda i: (i, 0, 0, 0)),
            pl.BlockSpec(y_table.shape, lambda i: (0, 0)),
            pl.BlockSpec(z_table.shape, lambda i: (0, 0)),
        ],
        out_specs=pl.BlockSpec((modes_y, channels, lanes), lambda i: (0, 0, 0)),
        out_shape=jax.ShapeDtypeStruct((modes_y, channels, lanes), F32),
        scratch_shapes=[
            pltpu.VMEM((channels * modes_y, wide), BF16),
            pltpu.VMEM((channels * modes_y, wide), BF16),
        ],
    )(grid_field, jnp.asarray(y_table), jnp.asarray(z_table))


def exchange_kernel(width_gx, width_col, with_core, *refs):
    if with_core:
        send_ref, core_ref, out_ref, core_out, sends, recvs, own, core_sends, core_recvs, core_own = refs
    else:
        send_ref, out_ref, sends, recvs, own = refs
    count = width_gx * width_col
    my_gx, my_col = lax.axis_index("gx"), lax.axis_index("col")
    me = my_gx * width_col + my_col
    barrier = pltpu.get_barrier_semaphore()

    def where(step):
        peer = lax.rem(me + step, count)
        return peer, (peer // width_col, lax.rem(peer, width_col))

    def greet(step, carry):
        pl.semaphore_signal(barrier, inc=1, device_id=where(step)[1], device_id_type=MESH)
        return carry

    lax.fori_loop(1, count, greet, 0)
    keep = pltpu.make_async_copy(send_ref.at[me], out_ref.at[me], own)
    keep.start()
    if with_core:
        core_keep = pltpu.make_async_copy(core_ref.at[my_col], core_out.at[my_col], core_own)
        core_keep.start()
    pl.semaphore_wait(barrier, count - 1)

    def block(step):
        peer, place = where(step)
        return pltpu.make_async_remote_copy(
            src_ref=send_ref.at[peer],
            dst_ref=out_ref.at[me],
            send_sem=sends.at[step],
            recv_sem=recvs.at[step],
            device_id=place,
            device_id_type=MESH,
        )

    def core_block(step):
        peer = lax.rem(my_col + step, width_col)
        return pltpu.make_async_remote_copy(
            src_ref=core_ref.at[peer],
            dst_ref=core_out.at[my_col],
            send_sem=core_sends.at[step],
            recv_sem=core_recvs.at[step],
            device_id=(my_gx, peer),
            device_id_type=MESH,
        )

    def start(step, carry):
        block(step).start()
        return carry

    lax.fori_loop(1, count, start, 0)
    if with_core:
        for step in range(1, width_col):
            core_block(step).start()

    def finish(step, carry):
        block(step).wait_send()
        source = lax.rem(me + count - step, count)
        pltpu.make_async_remote_copy(
            src_ref=send_ref.at[source],
            dst_ref=out_ref.at[source],
            send_sem=sends.at[step],
            recv_sem=recvs.at[step],
            device_id=(my_gx, my_col),
            device_id_type=MESH,
        ).wait_recv()
        return carry

    lax.fori_loop(1, count, finish, 0)
    keep.wait()
    if with_core:
        for step in range(1, width_col):
            core_block(step).wait_send()
            source = lax.rem(my_col + width_col - step, width_col)
            pltpu.make_async_remote_copy(
                src_ref=core_ref.at[source],
                dst_ref=core_out.at[source],
                send_sem=core_sends.at[step],
                recv_sem=core_recvs.at[step],
                device_id=(my_gx, my_col),
                device_id_type=MESH,
            ).wait_recv()
        core_keep.wait()


def exchange(width_gx, width_col, collective, *arrays):
    with_core = len(arrays) == 2
    count = width_gx * width_col
    dma = pltpu.SemaphoreType.DMA
    scratch = [dma((count,)), dma((count,)), dma]
    if with_core:
        scratch += [dma((width_col,)), dma((width_col,)), dma]
    return pl.pallas_call(
        functools.partial(exchange_kernel, width_gx, width_col, with_core),
        out_shape=[jax.ShapeDtypeStruct(a.shape, a.dtype) for a in arrays],
        in_specs=[VMEM] * len(arrays),
        out_specs=[VMEM] * len(arrays),
        scratch_shapes=scratch,
        compiler_params=pltpu.CompilerParams(collective_id=collective, has_side_effects=True),
    )(*arrays)


def middle_kernel(
    width_gx, modes_z, arrived_ref, core_ref, x_rows_ref, mask_ref, z_rows_ref, fore_ref, back_ref,
    out_ref, rank_ref, high_ref, low_ref, plane_ref,
):
    width_col, channels = core_ref.shape[0], arrived_ref.shape[1]
    lanes = arrived_ref.shape[2]
    lead = lanes // modes_z
    both_modes = back_ref.shape[1] // 3
    ranks = x_rows_ref.shape[1]
    core_rows = ranks // width_col

    def core_part(first, rows):
        return core_ref[:, first : first + rows, :].reshape(width_col * rows, lanes)

    at = 2 * core_rows
    in_rows = jnp.concatenate([core_part(at, channels), core_part(at + channels, channels)], 1)
    out_rows = core_part(at + 2 * channels, channels)
    in_high, in_low = split(in_rows)
    in_stack = jnp.concatenate([in_high, in_low, in_high], 0)
    for slab in range(width_gx):
        block = arrived_ref[slab * width_col : (slab + 1) * width_col].reshape(-1, lanes)
        high = block.astype(BF16).astype(F32)
        stacked = jnp.concatenate([high, high, block - high], 0)
        value = dot(stacked.T.astype(BF16), in_stack)
        rank_ref[:, slab * lead : (slab + 1) * lead, :] = value.reshape(modes_z, lead, ranks)
    for l in range(modes_z):
        high, low = split(rank_ref[l])
        value = dot(fore_ref[...], jnp.concatenate([high, low, high], 0))
        value = value * x_rows_ref[...] * mask_ref[:, l : l + 1]
        value = jnp.concatenate([value[:both_modes], value[both_modes:]], 1)
        rows = slice(l * both_modes, (l + 1) * both_modes)
        high_ref[rows], low_ref[rows] = split(value)
    core = jnp.concatenate([core_part(0, core_rows), core_part(core_rows, core_rows)], 0)
    core_high, core_low = split(core)
    both = dot(high_ref[...], jnp.concatenate([core_high, core_low], 1))
    mixed = both[:, :lanes] + both[:, lanes:] + dot(low_ref[...], core_high)
    for l in range(modes_z):
        value = mixed[l * both_modes : (l + 1) * both_modes] * z_rows_ref[l : l + 1]
        high, low = split(value)
        value = dot(back_ref[...], jnp.concatenate([high, low, high], 0))
        plane_ref[:, l] = value.reshape(width_gx, lead, lanes)
    out_high, out_low = split(out_rows)
    out_stack = jnp.concatenate([out_high, out_low], 0)
    count = out_high.shape[0]
    last = (((1,), (1,)), ((), ()))
    for slab in range(width_gx):
        high, low = split(plane_ref[slab].reshape(lanes, lanes))
        both = lax.dot_general(out_stack, high, last, preferred_element_type=F32)
        value = both[:count] + both[count:]
        value = value + lax.dot_general(out_high, low, last, preferred_element_type=F32)
        out_ref[slab * width_col : (slab + 1) * width_col] = value.reshape(
            width_col, channels, lanes
        )


def middle(arrived, cores, x_rows, mask, z_rows, grid_x, modes_x, modes_z, width_gx):
    fore, back = x_tables(grid_x, modes_x)
    lanes = arrived.shape[2]
    ranks = x_rows.shape[1]
    return pl.pallas_call(
        functools.partial(middle_kernel, width_gx, modes_z),
        out_shape=jax.ShapeDtypeStruct(arrived.shape, F32),
        in_specs=[VMEM] * 7,
        out_specs=VMEM,
        scratch_shapes=[
            pltpu.VMEM((modes_z, 2 * grid_x, ranks), F32),
            pltpu.VMEM((modes_z * 2 * modes_x, 2 * ranks), BF16),
            pltpu.VMEM((modes_z * 2 * modes_x, 2 * ranks), BF16),
            pltpu.VMEM((width_gx, modes_z, lanes // modes_z, lanes), F32),
        ],
    )(arrived, cores, x_rows, mask, z_rows, jnp.asarray(fore), jnp.asarray(back))


def inverse_kernel(spec_ref, y_ref, z_high_ref, z_low_ref, out_ref, high_ref, low_ref):
    channel = pl.program_id(0)
    modes_y, _, lanes = spec_ref.shape
    planes, grid_z = out_ref.shape[1], out_ref.shape[3]

    @pl.when(channel == 0)
    def _():
        values = jnp.swapaxes(spec_ref[...], 0, 1).reshape(-1, lanes)
        high, low = split(values)
        result = dot(high, z_high_ref[...]) + dot(high, z_low_ref[...])
        result = result + dot(low, z_high_ref[...])
        high_ref[...], low_ref[...] = split(result)

    rows = pl.ds(pl.multiple_of(channel * modes_y, modes_y), modes_y)
    high, low = high_ref[rows], low_ref[rows]

    def tall(values, plane):
        at = 2 * plane * grid_z
        return [values[:, at : at + grid_z], values[:, at + grid_z : at + 2 * grid_z]]

    stacks = []
    for plane in range(planes):
        high_part = tall(high, plane)
        stacks.append(jnp.concatenate(high_part + tall(low, plane) + high_part, 0))
    for plane in range(0, planes, 2):
        pair = stacks[plane : plane + 2]
        value = dot(y_ref[...], jnp.concatenate(pair, 1)).astype(BF16)
        for step in range(len(pair)):
            out_ref[0, plane + step] = value[:, step * grid_z : (step + 1) * grid_z]


def inverse(returned, planes, grid_y, grid_z, modes_z):
    modes_y, channels, _ = returned.shape
    y_table, z_high, z_low = inverse_tables(grid_y, grid_z, modes_y, modes_z, planes)
    wide = planes * 2 * grid_z
    return pl.pallas_call(
        inverse_kernel,
        grid=(channels,),
        in_specs=[
            pl.BlockSpec(returned.shape, lambda i: (0, 0, 0)),
            pl.BlockSpec(y_table.shape, lambda i: (0, 0)),
            pl.BlockSpec(z_high.shape, lambda i: (0, 0)),
            pl.BlockSpec(z_low.shape, lambda i: (0, 0)),
        ],
        out_specs=pl.BlockSpec((1, planes, grid_y, grid_z), lambda i: (i, 0, 0, 0)),
        out_shape=jax.ShapeDtypeStruct((channels, planes, grid_y, grid_z), BF16),
        scratch_shapes=[
            pltpu.VMEM((channels * modes_y, wide), BF16),
            pltpu.VMEM((channels * modes_y, wide), BF16),
        ],
    )(returned, jnp.asarray(y_table), jnp.asarray(z_high), jnp.asarray(z_low))


def row_device(
    grid_field, tucker_core, in_factor, out_factor, x_factor, y_factor, z_factor, kx_reach
):
    channels, planes, grid_y, grid_z = grid_field.shape
    modes_x, modes_y, modes_z = x_factor.shape[0], y_factor.shape[0], z_factor.shape[0]
    width_gx, width_col = lax.axis_size("gx"), lax.axis_size("col")
    slab = lax.axis_index("gx")
    row = slab * width_col + lax.axis_index("col")
    rank_out = out_factor.shape[1]
    rank_dev, rank_x, rank_z = tucker_core.shape[1], x_factor.shape[1], z_factor.shape[1]
    spectrum = forward(grid_field, modes_y, modes_z)
    y_rows = lax.dynamic_slice_in_dim(y_factor, slab * width_col, width_col)
    core = jnp.einsum("prsabe,db->dpares", tucker_core, y_rows, precision=lax.Precision.HIGHEST)
    core = core.reshape(width_col, 2 * rank_x * rank_dev, rank_z * rank_out)
    lanes = core.shape[2]
    in_wide = in_factor.reshape(channels, width_col, 1, rank_dev)
    in_wide = jnp.broadcast_to(in_wide, (channels, width_col, rank_x, rank_dev))
    in_wide = in_wide.reshape(channels, 2, lanes).swapaxes(0, 1).reshape(2 * channels, lanes)
    out_wide = jnp.tile(out_factor, (1, rank_z))
    factors = jnp.concatenate([in_wide, out_wide], 0)
    factors = jnp.broadcast_to(factors[None], (width_col,) + factors.shape)
    message = jnp.concatenate([core, factors], 1)
    arrived, cores = exchange(width_gx, width_col, 0, spectrum, message)
    x_rows = jnp.broadcast_to(x_factor[:, None, :, None], (modes_x, width_col, rank_x, rank_dev))
    x_rows = jnp.tile(x_rows.reshape(modes_x, -1), (4, 1))
    reach = lax.dynamic_slice_in_dim(kx_reach, row, 1)
    mask = (jnp.abs(slot_freq(modes_x))[:, None] < reach).astype(F32)
    z_rows = jnp.repeat(z_factor, rank_out, axis=1)
    sent = middle(
        arrived, cores, x_rows, jnp.tile(mask, (4, 1)), z_rows, planes * width_gx, modes_x,
        modes_z, width_gx,
    )
    (returned,) = exchange(width_gx, width_col, 1, sent)
    return inverse(returned, planes, grid_y, grid_z, modes_z)


def per_device(
    grid_field, tucker_core, in_factor, out_factor, x_factor, y_factor, z_factor, kx_reach
):
    planes, grid_z = grid_field.shape[1], grid_field.shape[3]
    modes_y, modes_z = y_factor.shape[0], z_factor.shape[0]
    devices = lax.axis_size("gx") * lax.axis_size("col")
    ranks = in_factor.shape[1] * x_factor.shape[1]
    row_each = (
        devices == modes_y
        and planes == 4
        and grid_z == 128
        and planes * 2 * modes_z == 128
        and ranks == 256
        and out_factor.shape[1] * z_factor.shape[1] == 128
    )
    device = row_device if row_each else plain_device
    return device(
        grid_field, tucker_core, in_factor, out_factor, x_factor, y_factor, z_factor, kx_reach
    )


def solution(mesh):
    return jax.shard_map(
        per_device,
        mesh=mesh,
        in_specs=(
            P("col", "gx", None, None),
            P(None, "col", None, None, None, None),
            P("col", None),
            P("col", None),
            P(),
            P(),
            P(),
            P(),
        ),
        out_specs=P("col", "gx", None, None),
        check_vma=False,
    )
```

```python
import functools
import math

import jax
import jax.numpy as jnp
import numpy as np
from jax import lax
from jax.experimental import pallas as pl
from jax.experimental.pallas import tpu as pltpu
from jax.sharding import PartitionSpec as P

MESH = pl.DeviceIdType.MESH
VMEM = pl.BlockSpec(memory_space=pltpu.VMEM)
F32 = jnp.float32
BF16 = jnp.bfloat16


def slot_freq(slot_count):
    slot_index = jnp.arange(slot_count, dtype=jnp.int32)
    return jnp.where(slot_index < slot_count // 2, slot_index, slot_index - slot_count)


def phase_table(positions, extent, slot_count, direction):
    phase_steps = positions[:, None] * slot_freq(slot_count)[None, :] % extent
    radians = 2.0 * math.pi / extent * phase_steps.astype(jnp.float32)
    norm_scale = 1.0 / math.sqrt(extent)
    cosine = jnp.cos(radians) * norm_scale
    sine_part = direction * jnp.sin(radians) * norm_scale
    return jnp.stack([jnp.stack([cosine, -sine_part], 1), jnp.stack([sine_part, cosine], 1)], 1)


def z_tables(grid_z, modes_z):
    z_index = jnp.arange(grid_z, dtype=jnp.int32)
    kz_index = jnp.arange(modes_z, dtype=jnp.int32)
    phase_steps = z_index[:, None] * kz_index[None, :] % grid_z
    radians = 2.0 * math.pi / grid_z * phase_steps.astype(jnp.float32)
    norm_scale = 1.0 / math.sqrt(grid_z)
    cosine = jnp.cos(radians) * norm_scale
    sine_part = jnp.sin(radians) * norm_scale
    forward = jnp.stack([cosine, -sine_part], 1)
    weight = jnp.where(kz_index == 0, 1.0, 2.0).astype(jnp.float32)
    backward = jnp.stack([(cosine * weight[None, :]).T, -(sine_part * weight[None, :]).T], 0)
    return (forward, backward)


def plain_device(
    grid_field, tucker_core, in_factor, out_factor, x_factor, y_factor, z_factor, kx_reach
):
    highest = lax.Precision.HIGHEST
    channels, planes, grid_y, grid_z = grid_field.shape
    modes_x = x_factor.shape[0]
    modes_y = y_factor.shape[0]
    modes_z = z_factor.shape[0]
    width_gx = lax.axis_size("gx")
    grid_x = planes * width_gx
    columns = modes_y * modes_z
    col_dev = columns // width_gx
    slab_index = lax.axis_index("gx")
    z_forward, z_backward = z_tables(grid_z, modes_z)
    y_forward = phase_table(jnp.arange(grid_y, dtype=jnp.int32), grid_y, modes_y, 1.0)
    x_forward = phase_table(jnp.arange(grid_x, dtype=jnp.int32), grid_x, modes_x, 1.0)
    values = grid_field.astype(jnp.float32)
    z_spectrum = jnp.einsum("cxyz,zpl->cxply", values, z_forward, precision=highest)
    y_spectrum = jnp.einsum("cxply,ypqj->qcxjl", z_spectrum, y_forward, precision=highest)
    y_spectrum = y_spectrum.reshape(2, channels, planes, columns)
    first_col = slab_index * col_dev
    reach_dev = lax.dynamic_slice_in_dim(kx_reach.reshape(-1), first_col, col_dev)
    kept_mask = (jnp.abs(slot_freq(modes_x))[:, None] < reach_dev[None, :]).astype(jnp.float32)
    arrived = lax.all_to_all(y_spectrum, "gx", split_axis=3, concat_axis=2, tiled=True)
    spectrum = jnp.einsum("pcxm,xpqk->qckm", arrived, x_forward, precision=highest)
    partial_value = jnp.einsum("qckm,cr->qrkm", spectrum, in_factor, precision=highest)
    amplitude = lax.psum_scatter(partial_value, "col", scatter_dimension=1, tiled=True)
    amplitude = amplitude * kept_mask[None, None]
    column = first_col + jnp.arange(col_dev, dtype=jnp.int32)
    pick_y = (column[:, None] // modes_z == jnp.arange(modes_y, dtype=jnp.int32)[None, :]).astype(
        jnp.float32
    )
    pick_z = (column[:, None] % modes_z == jnp.arange(modes_z, dtype=jnp.int32)[None, :]).astype(
        jnp.float32
    )
    y_rows = jnp.dot(pick_y, y_factor, precision=highest)
    z_rows = jnp.dot(pick_z, z_factor, precision=highest)
    core_cols = jnp.einsum("prsabe,mb,me->prsam", tucker_core, y_rows, z_rows, precision=highest)
    kernel = jnp.einsum("prsam,ka->prskm", core_cols, x_factor, precision=highest)
    mixed_re = jnp.einsum("rskm,rkm->skm", kernel[0], amplitude[0], precision=highest) - jnp.einsum(
        "rskm,rkm->skm", kernel[1], amplitude[1], precision=highest
    )
    mixed_im = jnp.einsum("rskm,rkm->skm", kernel[0], amplitude[1], precision=highest) + jnp.einsum(
        "rskm,rkm->skm", kernel[1], amplitude[0], precision=highest
    )
    mixed_sum = lax.psum(jnp.stack([mixed_re, mixed_im]), "col")
    out_spec = jnp.einsum("os,qskm->qokm", out_factor, mixed_sum, precision=highest)
    x_backward = phase_table(jnp.arange(grid_x, dtype=jnp.int32), grid_x, modes_x, -1.0)
    x_values = jnp.einsum("pckm,xpqk->qcxm", out_spec, x_backward, precision=highest)
    returned = lax.all_to_all(x_values, "gx", split_axis=2, concat_axis=3, tiled=True)
    returned = returned.reshape(2, channels, planes, modes_y, modes_z)
    y_backward = phase_table(jnp.arange(grid_y, dtype=jnp.int32), grid_y, modes_y, -1.0)
    y_values = jnp.einsum("pcxjl,ypqj->cxqly", returned, y_backward, precision=highest)
    result = jnp.einsum("cxqly,qlz->cxyz", y_values, z_backward, precision=highest)
    return result.astype(jnp.bfloat16)


def split_np(table):
    high = table.astype(np.float32).astype(BF16)
    low = (table - high.astype(np.float64)).astype(np.float32).astype(BF16)
    return high, low


def split(values):
    high = values.astype(BF16)
    return high, (values - high.astype(F32)).astype(BF16)


def freqs(slots):
    index = np.arange(slots)
    return np.where(index < slots // 2, index, index - slots)


def waves(extent, frequencies):
    steps = np.arange(extent)[:, None] * frequencies[None, :] % extent
    angle = 2.0 * np.pi / extent * steps
    return np.cos(angle) / math.sqrt(extent), np.sin(angle) / math.sqrt(extent)


def dot(a, b):
    return jnp.dot(a, b, preferred_element_type=F32)


def forward_tables(grid_y, grid_z, modes_y, modes_z, planes):
    cos_y, sin_y = waves(grid_y, freqs(modes_y))
    high, low = split_np(np.concatenate([cos_y.T, -sin_y.T], 0))
    y_table = np.concatenate([high, low], 0)
    cos_z, sin_z = waves(grid_z, np.arange(modes_z))
    table = np.zeros((planes, 2, grid_z, modes_z, planes, 2))
    for plane in range(planes):
        table[plane, 0, :, :, plane, 0] = cos_z
        table[plane, 0, :, :, plane, 1] = -sin_z
        table[plane, 1, :, :, plane, 0] = sin_z
        table[plane, 1, :, :, plane, 1] = cos_z
    high, low = split_np(table.reshape(planes * 2 * grid_z, -1))
    return y_table, np.concatenate([high, low], 1)


def inverse_tables(grid_y, grid_z, modes_y, modes_z, planes):
    cos_y, sin_y = waves(grid_y, freqs(modes_y))
    high, low = split_np(np.concatenate([cos_y, -sin_y], 1))
    y_table = np.concatenate([high, high, low], 1)
    cos_z, sin_z = waves(grid_z, np.arange(modes_z))
    weight = np.where(np.arange(modes_z) == 0, 1.0, 2.0)
    cos_z, sin_z = (cos_z * weight).T, (sin_z * weight).T
    table = np.zeros((modes_z, planes, 2, planes, 2, grid_z))
    for plane in range(planes):
        table[:, plane, 0, plane, 0, :] = cos_z
        table[:, plane, 1, plane, 0, :] = -sin_z
        table[:, plane, 0, plane, 1, :] = sin_z
        table[:, plane, 1, plane, 1, :] = cos_z
    high, low = split_np(table.reshape(modes_z * planes * 2, -1))
    return y_table, high, low


def x_tables(grid_x, modes_x):
    cos_x, sin_x = waves(grid_x, freqs(modes_x))
    real = np.stack([cos_x.T, sin_x.T], 2).reshape(modes_x, -1)
    imag = np.stack([-sin_x.T, cos_x.T], 2).reshape(modes_x, -1)
    high, low = split_np(np.concatenate([real, imag, -imag, real], 0))
    forward = np.concatenate([high, high, low], 1)
    real = np.concatenate([cos_x, -sin_x], 1)
    imag = np.concatenate([sin_x, cos_x], 1)
    high, low = split_np(np.stack([real, imag], 1).reshape(grid_x * 2, -1))
    backward = np.concatenate([high, high, low], 1)
    return forward, backward


def selectors(width_col, rank_x, rank_dev, rank_z, rank_out):
    wide = np.arange(width_col * rank_x * rank_dev)
    rank_in = wide // (rank_x * rank_dev) * rank_dev + wide % rank_dev
    x_pick = wide // rank_dev % rank_x == np.arange(rank_x)[:, None]
    in_pick = rank_in == np.arange(width_col * rank_dev)[:, None]
    slim = np.arange(rank_z * rank_out)
    z_pick = slim // rank_out == np.arange(rank_z)[:, None]
    out_pick = slim % rank_out == np.arange(rank_out)[:, None]
    return [pick.astype(np.float32) for pick in (x_pick, in_pick, z_pick, out_pick)]


def spread(values, pick, dim):
    return lax.dot_general(
        values, pick, (((dim,), (0,)), ((), ())), precision=lax.Precision.HIGHEST,
        preferred_element_type=F32,
    )


def fused_kernel(
    width_gx, width_col, field_ref, core_ref, in_ref, out_factor_ref, x_ref, z_ref, reach_ref,
    x_pick_ref, in_pick_ref, z_pick_ref, out_pick_ref, y_table_ref, z_table_ref, fore_ref, back_ref,
    out_ref, field, y_high, y_low, spec, arrived, cores, factor, factors, rank_ref, high_ref,
    low_ref, plane_ref, result_ref, field_sems, sends, recvs, core_sends, core_recvs, factor_sends,
    factor_recvs, back_sends, back_recvs, own,
):
    count = width_gx * width_col
    my_gx, my_col = lax.axis_index("gx"), lax.axis_index("col")
    me = my_gx * width_col + my_col
    channels, planes, _, grid_z = field.shape
    groups, modes_y, group, lanes = spec.shape
    modes_x, modes_z = x_ref.shape[1], z_ref.shape[1]
    barrier = pltpu.get_barrier_semaphore()

    def fetch(channel):
        return pltpu.make_async_copy(
            field_ref.at[channel], field.at[channel], field_sems.at[channel]
        )

    def begin(channel, carry):
        fetch(channel).start()
        return carry

    lax.fori_loop(0, channels, begin, 0)

    def place(peer):
        return peer // width_col, lax.rem(peer, width_col)

    def greet(step, carry):
        peer = lax.rem(me + step, count)
        pl.semaphore_signal(barrier, inc=1, device_id=place(peer), device_id_type=MESH)
        return carry

    lax.fori_loop(1, count, greet, 0)

    def remote(source, target, send_sem, recv_sem, device):
        return pltpu.make_async_remote_copy(
            src_ref=source, dst_ref=target, send_sem=send_sem, recv_sem=recv_sem,
            device_id=device, device_id_type=MESH,
        )

    in_wide = spread(in_ref[...], in_pick_ref[...], 1)
    factor[:channels] = in_wide[:, :lanes]
    factor[channels : 2 * channels] = in_wide[:, lanes:]
    factor[2 * channels :] = spread(out_factor_ref[...], out_pick_ref[...], 1)

    def spectrum_copy(part, peer, writer, device):
        return remote(
            spec.at[part, peer], arrived.at[part, writer], sends.at[part, peer],
            recvs.at[part, writer], device,
        )

    def core_copy(peer, writer, device):
        return remote(
            core_ref.at[peer], cores.at[writer], core_sends.at[peer], core_recvs.at[writer], device
        )

    def factor_copy(peer, writer, device):
        return remote(
            factor, factors.at[writer], factor_sends.at[peer], factor_recvs.at[writer], device
        )

    half = 2 * modes_y
    pair = 2
    for part in range(groups):

        def transform(step, carry, part=part):
            for offset in range(pair):
                local = step * pair + offset
                channel = part * group + local
                fetch(channel).wait()
                parts = []
                for plane in range(planes):
                    both = dot(y_table_ref[...], field[channel, plane])
                    y_values = both[:half] + both[half:]
                    parts += [y_values[:modes_y], y_values[modes_y:]]
                high, low = split(jnp.concatenate(parts, 1))
                rows = pl.ds(pl.multiple_of(local * modes_y, modes_y), modes_y)
                y_high[rows] = high
                y_low[rows] = low
            return carry

        lax.fori_loop(0, group // pair, transform, 0)
        both = dot(y_high[...], z_table_ref[...])
        value = both[:, :lanes] + both[:, lanes:] + dot(y_low[...], z_table_ref[:, :lanes])
        spec[part] = jnp.swapaxes(value.reshape(group, modes_y, lanes), 0, 1)
        if part == 0:
            pl.semaphore_wait(barrier, count - 1)
            for step in range(1, width_col):
                peer = lax.rem(my_col + step, width_col)
                factor_copy(peer, my_col, (my_gx, peer)).start()
                core_copy(peer, my_col, (my_gx, peer)).start()
            pltpu.make_async_copy(core_ref.at[my_col], cores.at[my_col], own.at[0]).start()
            pltpu.make_async_copy(factor, factors.at[my_col], own.at[1]).start()
        pltpu.make_async_copy(spec.at[part, me], arrived.at[part, me], own.at[3 + part]).start()

        def send(step, carry, part=part):
            peer = lax.rem(me + step, count)
            spectrum_copy(part, peer, me, place(peer)).start()
            return carry

        lax.fori_loop(1, count, send, 0)

    x_wide = spread(x_ref[...], x_pick_ref[...], 0)
    x_rows = jnp.concatenate([x_wide] * 4, 0)
    z_rows = spread(z_ref[...], z_pick_ref[...], 0)
    spot = lax.broadcasted_iota(jnp.int32, reach_ref.shape, 1)
    reach = jnp.where(spot == me, reach_ref[...].astype(F32), 0.0)
    reach = jnp.sum(reach, axis=1, keepdims=True)
    slot = lax.broadcasted_iota(jnp.int32, (modes_x, x_rows.shape[1]), 0)
    slot = jnp.where(slot < modes_x // 2, slot, modes_x - slot).astype(F32)
    slot = jnp.concatenate([slot] * 4, 0)

    for step in range(1, width_col):
        source = lax.rem(my_col + step, width_col)
        factor_copy(source, source, (my_gx, my_col)).wait_recv()
        core_copy(source, source, (my_gx, my_col)).wait_recv()
    pltpu.make_async_copy(core_ref.at[my_col], cores.at[my_col], own.at[0]).wait()
    pltpu.make_async_copy(factor, factors.at[my_col], own.at[1]).wait()

    lead = lanes // modes_z
    both_modes = 2 * modes_x
    ranks = x_rows.shape[1]
    core_rows = ranks // width_col

    def stacked_rows(ref, first, rows):
        return ref[:, first : first + rows, :].reshape(width_col * rows, lanes)

    in_rows = jnp.concatenate(
        [stacked_rows(factors, 0, channels), stacked_rows(factors, channels, channels)], 1
    )
    out_rows = stacked_rows(factors, 2 * channels, channels)
    in_high, in_low = split(in_rows)
    in_stack = jnp.concatenate([in_high, in_low, in_high], 0)
    core = jnp.concatenate(
        [stacked_rows(cores, 0, core_rows), stacked_rows(cores, core_rows, core_rows)], 0
    )
    core_high, core_low = split(core)
    core_both = jnp.concatenate([core_high, core_low], 1)
    out_high, out_low = split(out_rows)
    out_stack = jnp.concatenate([out_high, out_low], 0)

    for part in range(groups):
        pltpu.make_async_copy(spec.at[part, me], arrived.at[part, me], own.at[3 + part]).wait()

        def receive(step, carry, part=part):
            source = lax.rem(me + count - step, count)
            spectrum_copy(part, source, source, (my_gx, my_col)).wait_recv()
            return carry

        lax.fori_loop(1, count, receive, 0)

    for slab in range(width_gx):
        blocks = [
            arrived[part, slab * width_col + source]
            for source in range(width_col)
            for part in range(groups)
        ]
        block = jnp.concatenate(blocks, 0)
        high = block.astype(BF16).astype(F32)
        stacked = jnp.concatenate([high, high, block - high], 0)
        value = dot(stacked.T.astype(BF16), in_stack)
        rank_ref[:, slab * lead : (slab + 1) * lead, :] = value.reshape(modes_z, lead, ranks)
    for l in range(modes_z):
        high, low = split(rank_ref[l])
        value = dot(fore_ref[...], jnp.concatenate([high, low, high], 0))
        value = value * jnp.where(slot < reach[l : l + 1], x_rows, 0.0)
        value = jnp.concatenate([value[:both_modes], value[both_modes:]], 1)
        rows = slice(l * both_modes, (l + 1) * both_modes)
        high_ref[rows], low_ref[rows] = split(value)
    both = dot(high_ref[...], core_both)
    mixed = both[:, :lanes] + both[:, lanes:] + dot(low_ref[...], core_high)
    for l in range(modes_z):
        value = mixed[l * both_modes : (l + 1) * both_modes] * z_rows[l : l + 1]
        high, low = split(value)
        value = dot(back_ref[...], jnp.concatenate([high, low, high], 0))
        plane_ref[:, l] = value.reshape(width_gx, lead, lanes)

    def back_copy(peer, writer, device):
        return remote(
            result_ref.at[peer], out_ref.at[writer], back_sends.at[peer], back_recvs.at[writer],
            device,
        )

    rows_out = out_high.shape[0]
    last = (((1,), (1,)), ((), ()))

    def send_slab(slab):
        for step in range(width_col):
            peer_col = lax.rem(my_col + step, width_col)
            peer = slab * width_col + peer_col

            @pl.when(peer != me)
            def _(peer=peer, peer_col=peer_col):
                back_copy(peer, me, (slab, peer_col)).start()

    for step in range(width_gx):
        slab = lax.rem(my_gx + step, width_gx)
        high, low = split(plane_ref[slab].reshape(lanes, lanes))
        both = lax.dot_general(out_stack, high, last, preferred_element_type=F32)
        value = both[:rows_out] + both[rows_out:]
        value = value + lax.dot_general(out_high, low, last, preferred_element_type=F32)
        result_ref[pl.ds(slab * width_col, width_col)] = value.reshape(width_col, channels, lanes)
        if step > 0:
            send_slab(lax.rem(my_gx + step - 1, width_gx))
    send_slab(lax.rem(my_gx + width_gx - 1, width_gx))
    keep = pltpu.make_async_copy(result_ref.at[me], out_ref.at[me], own.at[2])
    keep.start()

    def finish_sends(step, carry):
        peer = lax.rem(me + step, count)
        for part in range(groups):
            spectrum_copy(part, peer, me, place(peer)).wait_send()
        return carry

    lax.fori_loop(1, count, finish_sends, 0)
    for step in range(1, width_col):
        peer = lax.rem(my_col + step, width_col)
        factor_copy(peer, my_col, (my_gx, peer)).wait_send()
        core_copy(peer, my_col, (my_gx, peer)).wait_send()

    def finish(step, carry):
        peer = lax.rem(me + step, count)
        back_copy(peer, me, place(peer)).wait_send()
        source = lax.rem(me + count - step, count)
        back_copy(source, source, (my_gx, my_col)).wait_recv()
        return carry

    lax.fori_loop(1, count, finish, 0)
    keep.wait()


def fused(
    grid_field, core, in_factor, out_factor, x_factor, z_factor, kx_reach, width_gx, width_col,
    rank_dev,
):
    channels, planes, grid_y, grid_z = grid_field.shape
    modes_x, rank_x = x_factor.shape
    modes_z, rank_z = z_factor.shape
    modes_y, rank_out = kx_reach.shape[0], out_factor.shape[1]
    y_table, z_table = forward_tables(grid_y, grid_z, modes_y, modes_z, planes)
    fore, back = x_tables(planes * width_gx, modes_x)
    picks = selectors(width_col, rank_x, rank_dev, rank_z, rank_out)
    count = width_gx * width_col
    lanes, wide = planes * 2 * modes_z, planes * 2 * grid_z
    ranks = width_col * rank_x * rank_dev
    group = 8
    groups = channels // group
    dma = pltpu.SemaphoreType.DMA
    tables = [jnp.asarray(t) for t in picks + [y_table, z_table, fore, back]]
    return pl.pallas_call(
        functools.partial(fused_kernel, width_gx, width_col),
        out_shape=jax.ShapeDtypeStruct((count, channels, lanes), F32),
        in_specs=[pl.BlockSpec(memory_space=pl.ANY)] + [VMEM] * (6 + len(tables)),
        out_specs=VMEM,
        scratch_shapes=[
            pltpu.VMEM(grid_field.shape, BF16),
            pltpu.VMEM((group * modes_y, wide), BF16),
            pltpu.VMEM((group * modes_y, wide), BF16),
            pltpu.VMEM((groups, modes_y, group, lanes), F32),
            pltpu.VMEM((groups, count, group, lanes), F32),
            pltpu.VMEM(core.shape, F32),
            pltpu.VMEM((3 * channels, lanes), F32),
            pltpu.VMEM((width_col, 3 * channels, lanes), F32),
            pltpu.VMEM((modes_z, 2 * planes * width_gx, ranks), F32),
            pltpu.VMEM((modes_z * 2 * modes_x, 2 * ranks), BF16),
            pltpu.VMEM((modes_z * 2 * modes_x, 2 * ranks), BF16),
            pltpu.VMEM((width_gx, modes_z, lanes // modes_z, lanes), F32),
            pltpu.VMEM((count, channels, lanes), F32),
            dma((channels,)),
            dma((groups, count)),
            dma((groups, count)),
            dma((width_col,)),
            dma((width_col,)),
            dma((width_col,)),
            dma((width_col,)),
            dma((count,)),
            dma((count,)),
            dma((3 + groups,)),
        ],
        compiler_params=pltpu.CompilerParams(
            collective_id=0, has_side_effects=True, vmem_limit_bytes=48 * 2**20
        ),
    )(grid_field, core, in_factor, out_factor, x_factor.T, z_factor.T, kx_reach.T, *tables)


def inverse_kernel(spec_ref, y_ref, z_high_ref, z_low_ref, out_ref, high_ref, low_ref):
    step = pl.program_id(0)
    modes_y, channels, lanes = spec_ref.shape
    block, planes, grid_z = out_ref.shape[0], out_ref.shape[1], out_ref.shape[3]
    group = 8
    for part in range(channels // group):

        @pl.when(step * block == part * group)
        def _(part=part):
            values = spec_ref[:, part * group : (part + 1) * group]
            values = jnp.swapaxes(values, 0, 1).reshape(-1, lanes)
            high, low = split(values)
            result = dot(high, z_high_ref[...]) + dot(high, z_low_ref[...])
            result = result + dot(low, z_high_ref[...])
            rows = slice(part * group * modes_y, (part + 1) * group * modes_y)
            high_ref[rows], low_ref[rows] = split(result)

    def tall(values, plane):
        at = 2 * plane * grid_z
        return [values[:, at : at + grid_z], values[:, at + grid_z : at + 2 * grid_z]]

    for local in range(block):
        first = (step * block + local) * modes_y
        rows = pl.ds(pl.multiple_of(first, modes_y), modes_y)
        high, low = high_ref[rows], low_ref[rows]
        stacks = []
        for plane in range(planes):
            high_part = tall(high, plane)
            stacks.append(jnp.concatenate(high_part + tall(low, plane) + high_part, 0))
        for plane in range(0, planes, 2):
            value = dot(y_ref[...], jnp.concatenate(stacks[plane : plane + 2], 1)).astype(BF16)
            out_ref[local, plane] = value[:, :grid_z]
            out_ref[local, plane + 1] = value[:, grid_z:]


def inverse(returned, planes, grid_y, grid_z, modes_z):
    modes_y, channels, _ = returned.shape
    y_table, z_high, z_low = inverse_tables(grid_y, grid_z, modes_y, modes_z, planes)
    wide = planes * 2 * grid_z
    block = 4
    return pl.pallas_call(
        inverse_kernel,
        grid=(channels // block,),
        in_specs=[
            pl.BlockSpec(returned.shape, lambda i: (0, 0, 0)),
            pl.BlockSpec(y_table.shape, lambda i: (0, 0)),
            pl.BlockSpec(z_high.shape, lambda i: (0, 0)),
            pl.BlockSpec(z_low.shape, lambda i: (0, 0)),
        ],
        out_specs=pl.BlockSpec((block, planes, grid_y, grid_z), lambda i: (i, 0, 0, 0)),
        out_shape=jax.ShapeDtypeStruct((channels, planes, grid_y, grid_z), BF16),
        scratch_shapes=[
            pltpu.VMEM((channels * modes_y, wide), BF16),
            pltpu.VMEM((channels * modes_y, wide), BF16),
        ],
    )(returned, jnp.asarray(y_table), jnp.asarray(z_high), jnp.asarray(z_low))


def row_device(
    grid_field, tucker_core, in_factor, out_factor, x_factor, y_factor, z_factor, kx_reach
):
    _, planes, grid_y, grid_z = grid_field.shape
    width_gx, width_col = lax.axis_size("gx"), lax.axis_size("col")
    rank_out = out_factor.shape[1]
    rank_dev, rank_x, rank_z = tucker_core.shape[1], x_factor.shape[1], z_factor.shape[1]
    y_rows = lax.dynamic_slice_in_dim(y_factor, lax.axis_index("gx") * width_col, width_col)
    core = jnp.einsum("prsabe,db->dpares", tucker_core, y_rows, precision=lax.Precision.HIGHEST)
    core = core.reshape(width_col, 2 * rank_x * rank_dev, rank_z * rank_out)
    returned = fused(
        grid_field, core, in_factor, out_factor, x_factor, z_factor, kx_reach, width_gx, width_col,
        rank_dev,
    )
    return inverse(returned, planes, grid_y, grid_z, z_factor.shape[0])


def per_device(
    grid_field, tucker_core, in_factor, out_factor, x_factor, y_factor, z_factor, kx_reach
):
    planes, grid_z = grid_field.shape[1], grid_field.shape[3]
    modes_y, modes_z = y_factor.shape[0], z_factor.shape[0]
    devices = lax.axis_size("gx") * lax.axis_size("col")
    ranks = in_factor.shape[1] * x_factor.shape[1]
    row_each = (
        devices == modes_y
        and planes == 4
        and grid_field.shape[0] % 8 == 0
        and grid_z == 128
        and planes * 2 * modes_z == 128
        and ranks == 256
        and out_factor.shape[1] * z_factor.shape[1] == 128
    )
    device = row_device if row_each else plain_device
    return device(
        grid_field, tucker_core, in_factor, out_factor, x_factor, y_factor, z_factor, kx_reach
    )


def solution(mesh):
    return jax.shard_map(
        per_device,
        mesh=mesh,
        in_specs=(
            P("col", "gx", None, None),
            P(None, "col", None, None, None, None),
            P("col", None),
            P("col", None),
            P(),
            P(),
            P(),
            P(),
        ),
        out_specs=P("col", "gx", None, None),
        check_vma=False,
    )
```

```python
import functools
import math

import jax
import jax.numpy as jnp
import numpy as np
from jax import lax
from jax.experimental import pallas as pl
from jax.experimental.pallas import tpu as pltpu
from jax.sharding import PartitionSpec as P

MESH = pl.DeviceIdType.MESH
VMEM = pl.BlockSpec(memory_space=pltpu.VMEM)
F32 = jnp.float32
BF16 = jnp.bfloat16


def slot_freq(slot_count):
    slot_index = jnp.arange(slot_count, dtype=jnp.int32)
    return jnp.where(slot_index < slot_count // 2, slot_index, slot_index - slot_count)


def phase_table(positions, extent, slot_count, direction):
    phase_steps = positions[:, None] * slot_freq(slot_count)[None, :] % extent
    radians = 2.0 * math.pi / extent * phase_steps.astype(jnp.float32)
    norm_scale = 1.0 / math.sqrt(extent)
    cosine = jnp.cos(radians) * norm_scale
    sine_part = direction * jnp.sin(radians) * norm_scale
    return jnp.stack([jnp.stack([cosine, -sine_part], 1), jnp.stack([sine_part, cosine], 1)], 1)


def z_tables(grid_z, modes_z):
    z_index = jnp.arange(grid_z, dtype=jnp.int32)
    kz_index = jnp.arange(modes_z, dtype=jnp.int32)
    phase_steps = z_index[:, None] * kz_index[None, :] % grid_z
    radians = 2.0 * math.pi / grid_z * phase_steps.astype(jnp.float32)
    norm_scale = 1.0 / math.sqrt(grid_z)
    cosine = jnp.cos(radians) * norm_scale
    sine_part = jnp.sin(radians) * norm_scale
    forward = jnp.stack([cosine, -sine_part], 1)
    weight = jnp.where(kz_index == 0, 1.0, 2.0).astype(jnp.float32)
    backward = jnp.stack([(cosine * weight[None, :]).T, -(sine_part * weight[None, :]).T], 0)
    return (forward, backward)


def plain_device(
    grid_field, tucker_core, in_factor, out_factor, x_factor, y_factor, z_factor, kx_reach
):
    highest = lax.Precision.HIGHEST
    channels, planes, grid_y, grid_z = grid_field.shape
    modes_x = x_factor.shape[0]
    modes_y = y_factor.shape[0]
    modes_z = z_factor.shape[0]
    width_gx = lax.axis_size("gx")
    grid_x = planes * width_gx
    columns = modes_y * modes_z
    col_dev = columns // width_gx
    slab_index = lax.axis_index("gx")
    z_forward, z_backward = z_tables(grid_z, modes_z)
    y_forward = phase_table(jnp.arange(grid_y, dtype=jnp.int32), grid_y, modes_y, 1.0)
    x_forward = phase_table(jnp.arange(grid_x, dtype=jnp.int32), grid_x, modes_x, 1.0)
    values = grid_field.astype(jnp.float32)
    z_spectrum = jnp.einsum("cxyz,zpl->cxply", values, z_forward, precision=highest)
    y_spectrum = jnp.einsum("cxply,ypqj->qcxjl", z_spectrum, y_forward, precision=highest)
    y_spectrum = y_spectrum.reshape(2, channels, planes, columns)
    first_col = slab_index * col_dev
    reach_dev = lax.dynamic_slice_in_dim(kx_reach.reshape(-1), first_col, col_dev)
    kept_mask = (jnp.abs(slot_freq(modes_x))[:, None] < reach_dev[None, :]).astype(jnp.float32)
    arrived = lax.all_to_all(y_spectrum, "gx", split_axis=3, concat_axis=2, tiled=True)
    spectrum = jnp.einsum("pcxm,xpqk->qckm", arrived, x_forward, precision=highest)
    partial_value = jnp.einsum("qckm,cr->qrkm", spectrum, in_factor, precision=highest)
    amplitude = lax.psum_scatter(partial_value, "col", scatter_dimension=1, tiled=True)
    amplitude = amplitude * kept_mask[None, None]
    column = first_col + jnp.arange(col_dev, dtype=jnp.int32)
    pick_y = (column[:, None] // modes_z == jnp.arange(modes_y, dtype=jnp.int32)[None, :]).astype(
        jnp.float32
    )
    pick_z = (column[:, None] % modes_z == jnp.arange(modes_z, dtype=jnp.int32)[None, :]).astype(
        jnp.float32
    )
    y_rows = jnp.dot(pick_y, y_factor, precision=highest)
    z_rows = jnp.dot(pick_z, z_factor, precision=highest)
    core_cols = jnp.einsum("prsabe,mb,me->prsam", tucker_core, y_rows, z_rows, precision=highest)
    kernel = jnp.einsum("prsam,ka->prskm", core_cols, x_factor, precision=highest)
    mixed_re = jnp.einsum("rskm,rkm->skm", kernel[0], amplitude[0], precision=highest) - jnp.einsum(
        "rskm,rkm->skm", kernel[1], amplitude[1], precision=highest
    )
    mixed_im = jnp.einsum("rskm,rkm->skm", kernel[0], amplitude[1], precision=highest) + jnp.einsum(
        "rskm,rkm->skm", kernel[1], amplitude[0], precision=highest
    )
    mixed_sum = lax.psum(jnp.stack([mixed_re, mixed_im]), "col")
    out_spec = jnp.einsum("os,qskm->qokm", out_factor, mixed_sum, precision=highest)
    x_backward = phase_table(jnp.arange(grid_x, dtype=jnp.int32), grid_x, modes_x, -1.0)
    x_values = jnp.einsum("pckm,xpqk->qcxm", out_spec, x_backward, precision=highest)
    returned = lax.all_to_all(x_values, "gx", split_axis=2, concat_axis=3, tiled=True)
    returned = returned.reshape(2, channels, planes, modes_y, modes_z)
    y_backward = phase_table(jnp.arange(grid_y, dtype=jnp.int32), grid_y, modes_y, -1.0)
    y_values = jnp.einsum("pcxjl,ypqj->cxqly", returned, y_backward, precision=highest)
    result = jnp.einsum("cxqly,qlz->cxyz", y_values, z_backward, precision=highest)
    return result.astype(jnp.bfloat16)


def split_np(table):
    high = table.astype(np.float32).astype(BF16)
    low = (table - high.astype(np.float64)).astype(np.float32).astype(BF16)
    return high, low


def split(values):
    high = values.astype(BF16)
    return high, (values - high.astype(F32)).astype(BF16)


def freqs(slots):
    index = np.arange(slots)
    return np.where(index < slots // 2, index, index - slots)


def waves(extent, frequencies):
    steps = np.arange(extent)[:, None] * frequencies[None, :] % extent
    angle = 2.0 * np.pi / extent * steps
    return np.cos(angle) / math.sqrt(extent), np.sin(angle) / math.sqrt(extent)


def dot(a, b):
    return jnp.dot(a, b, preferred_element_type=F32)


def forward_tables(grid_y, grid_z, modes_y, modes_z, planes):
    cos_y, sin_y = waves(grid_y, freqs(modes_y))
    high, low = split_np(np.concatenate([cos_y.T, -sin_y.T], 0))
    y_table = np.concatenate([high, low], 0)
    cos_z, sin_z = waves(grid_z, np.arange(modes_z))
    table = np.zeros((planes, 2, grid_z, modes_z, planes, 2))
    for plane in range(planes):
        table[plane, 0, :, :, plane, 0] = cos_z
        table[plane, 0, :, :, plane, 1] = -sin_z
        table[plane, 1, :, :, plane, 0] = sin_z
        table[plane, 1, :, :, plane, 1] = cos_z
    high, low = split_np(table.reshape(planes * 2 * grid_z, -1))
    return y_table, np.concatenate([high, low], 1)


def inverse_tables(grid_y, grid_z, modes_y, modes_z, planes):
    cos_y, sin_y = waves(grid_y, freqs(modes_y))
    high, low = split_np(np.concatenate([cos_y, -sin_y], 1))
    y_table = np.concatenate([high, high, low], 1)
    cos_z, sin_z = waves(grid_z, np.arange(modes_z))
    weight = np.where(np.arange(modes_z) == 0, 1.0, 2.0)
    cos_z, sin_z = (cos_z * weight).T, (sin_z * weight).T
    table = np.zeros((modes_z, planes, 2, planes, 2, grid_z))
    for plane in range(planes):
        table[:, plane, 0, plane, 0, :] = cos_z
        table[:, plane, 1, plane, 0, :] = -sin_z
        table[:, plane, 0, plane, 1, :] = sin_z
        table[:, plane, 1, plane, 1, :] = cos_z
    high, low = split_np(table.reshape(modes_z * planes * 2, -1))
    return y_table, high, low


def x_tables(grid_x, modes_x):
    cos_x, sin_x = waves(grid_x, freqs(modes_x))
    real = np.stack([cos_x.T, sin_x.T], 2).reshape(modes_x, -1)
    imag = np.stack([-sin_x.T, cos_x.T], 2).reshape(modes_x, -1)
    high, low = split_np(np.concatenate([real, imag, -imag, real], 0))
    forward = np.concatenate([high, high, low], 1)
    real = np.concatenate([cos_x, -sin_x], 1)
    imag = np.concatenate([sin_x, cos_x], 1)
    high, low = split_np(np.stack([real, imag], 1).reshape(grid_x * 2, -1))
    backward = np.concatenate([high, high, low], 1)
    return forward, backward


def selectors(width_col, rank_x, rank_dev, rank_z, rank_out):
    wide = np.arange(width_col * rank_x * rank_dev)
    rank_in = wide // (rank_x * rank_dev) * rank_dev + wide % rank_dev
    x_pick = wide // rank_dev % rank_x == np.arange(rank_x)[:, None]
    in_pick = rank_in == np.arange(width_col * rank_dev)[:, None]
    slim = np.arange(rank_z * rank_out)
    z_pick = slim // rank_out == np.arange(rank_z)[:, None]
    out_pick = slim % rank_out == np.arange(rank_out)[:, None]
    return [pick.astype(np.float32) for pick in (x_pick, in_pick, z_pick, out_pick)]


def spread(values, pick, dim):
    return lax.dot_general(
        values, pick, (((dim,), (0,)), ((), ())), precision=lax.Precision.HIGHEST,
        preferred_element_type=F32,
    )


def fused_kernel(
    width_gx, width_col, field_ref, core_ref, in_ref, out_factor_ref, x_ref, z_ref, reach_ref,
    x_pick_ref, in_pick_ref, z_pick_ref, out_pick_ref, y_table_ref, z_table_ref, fore_ref, back_ref,
    out_ref, field, y_high, y_low, spec, arrived, cores, factor, factors, rank_ref, high_ref,
    low_ref, plane_ref, result_ref, field_sems, sends, recvs, core_sends, core_recvs, factor_sends,
    factor_recvs, back_sends, back_recvs, own,
):
    count = width_gx * width_col
    my_gx, my_col = lax.axis_index("gx"), lax.axis_index("col")
    me = my_gx * width_col + my_col
    channels, planes, _, grid_z = field.shape
    groups, modes_y, group, lanes = spec.shape
    modes_x, modes_z = x_ref.shape[1], z_ref.shape[1]
    barrier = pltpu.get_barrier_semaphore()

    def fetch(channel):
        return pltpu.make_async_copy(
            field_ref.at[channel], field.at[channel], field_sems.at[channel]
        )

    def begin(channel, carry):
        fetch(channel).start()
        return carry

    lax.fori_loop(0, channels, begin, 0)

    def place(peer):
        return peer // width_col, lax.rem(peer, width_col)

    def greet(step, carry):
        peer = lax.rem(me + step, count)
        pl.semaphore_signal(barrier, inc=1, device_id=place(peer), device_id_type=MESH)
        return carry

    lax.fori_loop(1, count, greet, 0)

    def remote(source, target, send_sem, recv_sem, device):
        return pltpu.make_async_remote_copy(
            src_ref=source, dst_ref=target, send_sem=send_sem, recv_sem=recv_sem,
            device_id=device, device_id_type=MESH,
        )

    in_wide = spread(in_ref[...], in_pick_ref[...], 1)
    factor[:channels] = in_wide[:, :lanes]
    factor[channels : 2 * channels] = in_wide[:, lanes:]
    factor[2 * channels :] = spread(out_factor_ref[...], out_pick_ref[...], 1)

    def spectrum_copy(part, peer, writer, device):
        return remote(
            spec.at[part, peer], arrived.at[part, writer], sends.at[part, peer],
            recvs.at[part, writer], device,
        )

    def core_copy(peer, writer, device):
        return remote(
            core_ref.at[peer], cores.at[writer], core_sends.at[peer], core_recvs.at[writer], device
        )

    def factor_copy(peer, writer, device):
        return remote(
            factor, factors.at[writer], factor_sends.at[peer], factor_recvs.at[writer], device
        )

    half = 2 * modes_y
    pair = 2
    for part in range(groups):

        def transform(step, carry, part=part):
            for offset in range(pair):
                local = step * pair + offset
                channel = part * group + local
                fetch(channel).wait()
                parts = []
                for plane in range(planes):
                    both = dot(y_table_ref[...], field[channel, plane])
                    y_values = both[:half] + both[half:]
                    parts += [y_values[:modes_y], y_values[modes_y:]]
                high, low = split(jnp.concatenate(parts, 1))
                rows = pl.ds(pl.multiple_of(local * modes_y, modes_y), modes_y)
                y_high[rows] = high
                y_low[rows] = low
            return carry

        lax.fori_loop(0, group // pair, transform, 0)
        both = dot(y_high[...], z_table_ref[...])
        value = both[:, :lanes] + both[:, lanes:] + dot(y_low[...], z_table_ref[:, :lanes])
        spec[part] = jnp.swapaxes(value.reshape(group, modes_y, lanes), 0, 1)
        if part == 0:
            pl.semaphore_wait(barrier, count - 1)
            for step in range(1, width_col):
                peer = lax.rem(my_col + step, width_col)
                factor_copy(peer, my_col, (my_gx, peer)).start()
                core_copy(peer, my_col, (my_gx, peer)).start()
            pltpu.make_async_copy(core_ref.at[my_col], cores.at[my_col], own.at[0]).start()
            pltpu.make_async_copy(factor, factors.at[my_col], own.at[1]).start()
        pltpu.make_async_copy(spec.at[part, me], arrived.at[part, me], own.at[3 + part]).start()

        def send(step, carry, part=part):
            peer = lax.rem(me + step, count)
            spectrum_copy(part, peer, me, place(peer)).start()
            return carry

        lax.fori_loop(1, count, send, 0)

    x_wide = spread(x_ref[...], x_pick_ref[...], 0)
    x_rows = jnp.concatenate([x_wide] * 4, 0)
    z_rows = spread(z_ref[...], z_pick_ref[...], 0)
    spot = lax.broadcasted_iota(jnp.int32, reach_ref.shape, 1)
    reach = jnp.where(spot == me, reach_ref[...].astype(F32), 0.0)
    reach = jnp.sum(reach, axis=1, keepdims=True)
    slot = lax.broadcasted_iota(jnp.int32, (modes_x, x_rows.shape[1]), 0)
    slot = jnp.where(slot < modes_x // 2, slot, modes_x - slot).astype(F32)
    slot = jnp.concatenate([slot] * 4, 0)

    for step in range(1, width_col):
        source = lax.rem(my_col + step, width_col)
        factor_copy(source, source, (my_gx, my_col)).wait_recv()
        core_copy(source, source, (my_gx, my_col)).wait_recv()
    pltpu.make_async_copy(core_ref.at[my_col], cores.at[my_col], own.at[0]).wait()
    pltpu.make_async_copy(factor, factors.at[my_col], own.at[1]).wait()

    lead = lanes // modes_z
    both_modes = 2 * modes_x
    ranks = x_rows.shape[1]
    core_rows = ranks // width_col

    def stacked_rows(ref, first, rows):
        return ref[:, first : first + rows, :].reshape(width_col * rows, lanes)

    in_rows = jnp.concatenate(
        [stacked_rows(factors, 0, channels), stacked_rows(factors, channels, channels)], 1
    )
    out_rows = stacked_rows(factors, 2 * channels, channels)
    in_high, in_low = split(in_rows)
    in_stack = jnp.concatenate([in_high, in_low, in_high], 0)
    core = jnp.concatenate(
        [stacked_rows(cores, 0, core_rows), stacked_rows(cores, core_rows, core_rows)], 0
    )
    core_high, core_low = split(core)
    core_both = jnp.concatenate([core_high, core_low], 1)
    out_high, out_low = split(out_rows)
    out_stack = jnp.concatenate([out_high, out_low], 0)

    for part in range(groups):
        pltpu.make_async_copy(spec.at[part, me], arrived.at[part, me], own.at[3 + part]).wait()

        def receive(step, carry, part=part):
            source = lax.rem(me + count - step, count)
            spectrum_copy(part, source, source, (my_gx, my_col)).wait_recv()
            return carry

        lax.fori_loop(1, count, receive, 0)

    for slab in range(width_gx):
        blocks = [
            arrived[part, slab * width_col + source]
            for source in range(width_col)
            for part in range(groups)
        ]
        block = jnp.concatenate(blocks, 0)
        high = block.astype(BF16).astype(F32)
        stacked = jnp.concatenate([high, high, block - high], 0)
        value = dot(stacked.T.astype(BF16), in_stack)
        rank_ref[:, slab * lead : (slab + 1) * lead, :] = value.reshape(modes_z, lead, ranks)
    for l in range(modes_z):
        high, low = split(rank_ref[l])
        value = dot(fore_ref[...], jnp.concatenate([high, low, high], 0))
        value = value * jnp.where(slot < reach[l : l + 1], x_rows, 0.0)
        value = jnp.concatenate([value[:both_modes], value[both_modes:]], 1)
        rows = slice(l * both_modes, (l + 1) * both_modes)
        high_ref[rows], low_ref[rows] = split(value)
    both = dot(high_ref[...], core_both)
    mixed = both[:, :lanes] + both[:, lanes:] + dot(low_ref[...], core_high)
    for l in range(modes_z):
        value = mixed[l * both_modes : (l + 1) * both_modes] * z_rows[l : l + 1]
        high, low = split(value)
        value = dot(back_ref[...], jnp.concatenate([high, low, high], 0))
        plane_ref[:, l] = value.reshape(width_gx, lead, lanes)

    def back_copy(peer, writer, device):
        return remote(
            result_ref.at[peer], out_ref.at[writer], back_sends.at[peer], back_recvs.at[writer],
            device,
        )

    rows_out = out_high.shape[0]
    last = (((1,), (1,)), ((), ()))

    def send_slab(slab):
        for step in range(width_col):
            peer_col = lax.rem(my_col + step, width_col)
            peer = slab * width_col + peer_col

            @pl.when(peer != me)
            def _(peer=peer, peer_col=peer_col):
                back_copy(peer, me, (slab, peer_col)).start()

    for step in range(width_gx):
        slab = lax.rem(my_gx + step, width_gx)
        high, low = split(plane_ref[slab].reshape(lanes, lanes))
        both = lax.dot_general(out_stack, high, last, preferred_element_type=F32)
        value = both[:rows_out] + both[rows_out:]
        value = value + lax.dot_general(out_high, low, last, preferred_element_type=F32)
        result_ref[pl.ds(slab * width_col, width_col)] = value.reshape(width_col, channels, lanes)
        if step > 0:
            send_slab(lax.rem(my_gx + step - 1, width_gx))
    send_slab(lax.rem(my_gx + width_gx - 1, width_gx))
    keep = pltpu.make_async_copy(result_ref.at[me], out_ref.at[me], own.at[2])
    keep.start()

    def finish_sends(step, carry):
        peer = lax.rem(me + step, count)
        for part in range(groups):
            spectrum_copy(part, peer, me, place(peer)).wait_send()
        return carry

    lax.fori_loop(1, count, finish_sends, 0)
    for step in range(1, width_col):
        peer = lax.rem(my_col + step, width_col)
        factor_copy(peer, my_col, (my_gx, peer)).wait_send()
        core_copy(peer, my_col, (my_gx, peer)).wait_send()

    def finish(step, carry):
        peer = lax.rem(me + step, count)
        back_copy(peer, me, place(peer)).wait_send()
        source = lax.rem(me + count - step, count)
        back_copy(source, source, (my_gx, my_col)).wait_recv()
        return carry

    lax.fori_loop(1, count, finish, 0)
    keep.wait()


def fused(
    grid_field, core, in_factor, out_factor, x_factor, z_factor, kx_reach, width_gx, width_col,
    rank_dev,
):
    channels, planes, grid_y, grid_z = grid_field.shape
    modes_x, rank_x = x_factor.shape
    modes_z, rank_z = z_factor.shape
    modes_y, rank_out = kx_reach.shape[0], out_factor.shape[1]
    y_table, z_table = forward_tables(grid_y, grid_z, modes_y, modes_z, planes)
    fore, back = x_tables(planes * width_gx, modes_x)
    picks = selectors(width_col, rank_x, rank_dev, rank_z, rank_out)
    count = width_gx * width_col
    lanes, wide = planes * 2 * modes_z, planes * 2 * grid_z
    ranks = width_col * rank_x * rank_dev
    group = 8
    groups = channels // group
    dma = pltpu.SemaphoreType.DMA
    tables = [jnp.asarray(t) for t in picks + [y_table, z_table, fore, back]]
    return pl.pallas_call(
        functools.partial(fused_kernel, width_gx, width_col),
        out_shape=jax.ShapeDtypeStruct((count, channels, lanes), F32),
        in_specs=[pl.BlockSpec(memory_space=pltpu.HBM)] + [VMEM] * (6 + len(tables)),
        out_specs=VMEM,
        scratch_shapes=[
            pltpu.VMEM(grid_field.shape, BF16),
            pltpu.VMEM((group * modes_y, wide), BF16),
            pltpu.VMEM((group * modes_y, wide), BF16),
            pltpu.VMEM((groups, modes_y, group, lanes), F32),
            pltpu.VMEM((groups, count, group, lanes), F32),
            pltpu.VMEM(core.shape, F32),
            pltpu.VMEM((3 * channels, lanes), F32),
            pltpu.VMEM((width_col, 3 * channels, lanes), F32),
            pltpu.VMEM((modes_z, 2 * planes * width_gx, ranks), F32),
            pltpu.VMEM((modes_z * 2 * modes_x, 2 * ranks), BF16),
            pltpu.VMEM((modes_z * 2 * modes_x, 2 * ranks), BF16),
            pltpu.VMEM((width_gx, modes_z, lanes // modes_z, lanes), F32),
            pltpu.VMEM((count, channels, lanes), F32),
            dma((channels,)),
            dma((groups, count)),
            dma((groups, count)),
            dma((width_col,)),
            dma((width_col,)),
            dma((width_col,)),
            dma((width_col,)),
            dma((count,)),
            dma((count,)),
            dma((3 + groups,)),
        ],
        compiler_params=pltpu.CompilerParams(
            collective_id=0, has_side_effects=True, vmem_limit_bytes=48 * 2**20
        ),
    )(grid_field, core, in_factor, out_factor, x_factor.T, z_factor.T, kx_reach.T, *tables)


def inverse_kernel(spec_ref, y_ref, z_high_ref, z_low_ref, out_ref, high_ref, low_ref):
    step = pl.program_id(0)
    modes_y, channels, lanes = spec_ref.shape
    block, planes, grid_z = out_ref.shape[0], out_ref.shape[1], out_ref.shape[3]
    group = 8
    for part in range(channels // group):

        @pl.when(step * block == part * group)
        def _(part=part):
            values = spec_ref[:, part * group : (part + 1) * group]
            values = jnp.swapaxes(values, 0, 1).reshape(-1, lanes)
            high, low = split(values)
            result = dot(high, z_high_ref[...]) + dot(high, z_low_ref[...])
            result = result + dot(low, z_high_ref[...])
            rows = slice(part * group * modes_y, (part + 1) * group * modes_y)
            high_ref[rows], low_ref[rows] = split(result)

    def tall(values, plane):
        at = 2 * plane * grid_z
        return [values[:, at : at + grid_z], values[:, at + grid_z : at + 2 * grid_z]]

    for local in range(block):
        first = (step * block + local) * modes_y
        rows = pl.ds(pl.multiple_of(first, modes_y), modes_y)
        high, low = high_ref[rows], low_ref[rows]
        stacks = []
        for plane in range(planes):
            high_part = tall(high, plane)
            stacks.append(jnp.concatenate(high_part + tall(low, plane) + high_part, 0))
        for plane in range(0, planes, 2):
            value = dot(y_ref[...], jnp.concatenate(stacks[plane : plane + 2], 1)).astype(BF16)
            out_ref[local, plane] = value[:, :grid_z]
            out_ref[local, plane + 1] = value[:, grid_z:]


def inverse(returned, planes, grid_y, grid_z, modes_z):
    modes_y, channels, _ = returned.shape
    y_table, z_high, z_low = inverse_tables(grid_y, grid_z, modes_y, modes_z, planes)
    wide = planes * 2 * grid_z
    block = 4
    return pl.pallas_call(
        inverse_kernel,
        grid=(channels // block,),
        in_specs=[
            pl.BlockSpec(returned.shape, lambda i: (0, 0, 0)),
            pl.BlockSpec(y_table.shape, lambda i: (0, 0)),
            pl.BlockSpec(z_high.shape, lambda i: (0, 0)),
            pl.BlockSpec(z_low.shape, lambda i: (0, 0)),
        ],
        out_specs=pl.BlockSpec((block, planes, grid_y, grid_z), lambda i: (i, 0, 0, 0)),
        out_shape=jax.ShapeDtypeStruct((channels, planes, grid_y, grid_z), BF16),
        scratch_shapes=[
            pltpu.VMEM((channels * modes_y, wide), BF16),
            pltpu.VMEM((channels * modes_y, wide), BF16),
        ],
    )(returned, jnp.asarray(y_table), jnp.asarray(z_high), jnp.asarray(z_low))


def row_device(
    grid_field, tucker_core, in_factor, out_factor, x_factor, y_factor, z_factor, kx_reach
):
    _, planes, grid_y, grid_z = grid_field.shape
    width_gx, width_col = lax.axis_size("gx"), lax.axis_size("col")
    rank_out = out_factor.shape[1]
    rank_dev, rank_x, rank_z = tucker_core.shape[1], x_factor.shape[1], z_factor.shape[1]
    y_rows = lax.dynamic_slice_in_dim(y_factor, lax.axis_index("gx") * width_col, width_col)
    core = jnp.einsum("prsabe,db->dpares", tucker_core, y_rows, precision=lax.Precision.HIGHEST)
    core = core.reshape(width_col, 2 * rank_x * rank_dev, rank_z * rank_out)
    returned = fused(
        grid_field, core, in_factor, out_factor, x_factor, z_factor, kx_reach, width_gx, width_col,
        rank_dev,
    )
    return inverse(returned, planes, grid_y, grid_z, z_factor.shape[0])


def per_device(
    grid_field, tucker_core, in_factor, out_factor, x_factor, y_factor, z_factor, kx_reach
):
    planes, grid_z = grid_field.shape[1], grid_field.shape[3]
    modes_y, modes_z = y_factor.shape[0], z_factor.shape[0]
    devices = lax.axis_size("gx") * lax.axis_size("col")
    ranks = in_factor.shape[1] * x_factor.shape[1]
    row_each = (
        devices == modes_y
        and planes == 4
        and grid_field.shape[0] % 8 == 0
        and grid_z == 128
        and planes * 2 * modes_z == 128
        and ranks == 256
        and out_factor.shape[1] * z_factor.shape[1] == 128
    )
    device = row_device if row_each else plain_device
    return device(
        grid_field, tucker_core, in_factor, out_factor, x_factor, y_factor, z_factor, kx_reach
    )


def solution(mesh):
    return jax.shard_map(
        per_device,
        mesh=mesh,
        in_specs=(
            P("col", "gx", None, None),
            P(None, "col", None, None, None, None),
            P("col", None),
            P("col", None),
            P(),
            P(),
            P(),
            P(),
        ),
        out_specs=P("col", "gx", None, None),
        check_vma=False,
    )
```
